512 devices in a mesh: frames: 32 (over y, x, core), heads: 16 (over z).
Axes of the slice: x: 4, y: 4, z: 16, core: 2. Of those that a mesh axis runs over, the one named last changes fastest.
Arguments:
- frames: bfloat16 [32768, 1152], P('frames', 'heads'), may hold values from -6 to 6
- latents: bfloat16 [256, 1152], P('frames'), may hold values from -400 to 400
- w_query: bfloat16 [1152, 4096], P(None, 'heads'), may hold values from -0.1875 to 0.1875
- w_key: bfloat16 [1152, 4096], P(None, 'heads'), may hold values from -0.1875 to 0.1875
- w_value: bfloat16 [1152, 4096], P(None, 'heads'), may hold values from -0.1875 to 0.1875
- w_out: bfloat16 [4096, 8192], P('heads', 'frames'), may hold values from -0.09375 to 0.09375
- norm_gain: float32 [8192], P('frames'), may hold values from 0.5 to 1.5
- w_gate: bfloat16 [8192, 16384], P('frames', 'heads'), may hold values from -0.0625 to 0.0625
- w_up: bfloat16 [8192, 16384], P('frames', 'heads'), may hold values from -0.0625 to 0.0625
- w_down: bfloat16 [16384, 8192], P('heads', 'frames'), may hold values from -0.046875 to 0.046875
Outputs:
- block_out: bfloat16 [256, 8192], P('heads', 'frames')
The draws below stay inside these ranges and needn't reach their ends.
All inputs are finite; a program needn't handle non-finite values.
Results may differ from the reference program's by a relative error of at most 0.023.
Values may be sent and summed in bfloat16 or wider, within the bound.
No kernel may reach another device: no remote copies, remote signals or barrier semaphores. Data moves between devices by JAX's collectives and lax.ppermute only.
A program may use at most 64 MiB of HBM per device.

```python
import jax
import jax.numpy as jnp
from jax import lax

VIS = 1152
NHEAD = 32
HDIM = 128
D = 8192
FF = 16384
LAT = 256
TOKENS = 32768
INNER = 4096


def draw_latents(key, part):
    base = jnp.clip(jax.random.normal(key, (LAT, VIS), jnp.float32), -6.0, 6.0)
    return base.astype(jnp.bfloat16)


def levels(rng, shape, cuts, smallest, top_value):
    def one(axis_at, parts):
        heights = jax.random.uniform(jax.random.fold_in(jax.random.fold_in(rng, 6), axis_at), (parts,), jnp.float32, smallest / len(cuts), top_value / len(cuts))
        return jnp.repeat(jnp.exp(heights), shape[axis_at] // parts).reshape((-1,) + (1,) * (len(shape) - axis_at - 1))

    gain = one(*cuts[0])
    for cut in cuts[1:]:
        gain = gain * one(*cut)
    return gain


def scatter_about(stream_key, shape, scale, bound, split=(), dtype=jnp.bfloat16):
    result = jax.random.normal(stream_key, shape, jnp.float32) * scale
    if len(split) > 0:
        result = levels(stream_key, shape, split, -0.22, 0.18) * result
    return jnp.clip(result, min=-bound, max=bound).astype(dtype)


def setup_inputs(seed: int = 0) -> dict:
    arg_keys = jax.random.split(jax.random.key(seed), 11)
    frames = scatter_about(arg_keys[0], (TOKENS, VIS), 1.0, 6.0, ((0, 32), (1, 16)))
    latents = draw_latents(jax.random.fold_in(arg_keys[10], 71), 0)
    w_query = scatter_about(arg_keys[2], (VIS, INNER), VIS ** -0.5, 0.1875, ((1, 16),))
    w_key = scatter_about(arg_keys[3], (VIS, INNER), VIS ** -0.5, 0.1875, ((1, 16),))
    w_value = scatter_about(arg_keys[4], (VIS, INNER), VIS ** -0.5, 0.1875, ((1, 16),))
    w_out = scatter_about(arg_keys[5], (INNER, D), INNER ** -0.5, 0.09375, ((0, 16), (1, 32)))
    norm_gain = jnp.clip(1.0 + 0.1 * jax.random.normal(arg_keys[6], (D,), jnp.float32), 0.5, 1.5)
    w_gate = scatter_about(arg_keys[7], (D, FF), D ** -0.5, 0.0625, ((0, 32), (1, 16)))
    w_up = scatter_about(arg_keys[8], (D, FF), D ** -0.5, 0.0625, ((0, 32), (1, 16)))
    w_down = scatter_about(arg_keys[9], (FF, D), FF ** -0.5, 0.046875, ((0, 16), (1, 32)))
    return dict(frames=frames, latents=latents, w_query=w_query, w_key=w_key, w_value=w_value, w_out=w_out, norm_gain=norm_gain, w_gate=w_gate, w_up=w_up, w_down=w_down)


norm_eps = 1e-06

def reference(frames, latents, w_query, w_key, w_value, w_out, norm_gain, w_gate, w_up, w_down):
    queries = jnp.dot(latents, w_query, preferred_element_type=jnp.float32).astype(jnp.bfloat16)
    query_heads = queries.reshape(LAT, NHEAD, HDIM).transpose(1, 0, 2)
    key_weights = w_key.reshape(VIS, NHEAD, HDIM).transpose(1, 0, 2)
    value_weights = w_value.reshape(VIS, NHEAD, HDIM).transpose(1, 0, 2)

    def attend(inputs):
        query_head, key_weight, value_weight = inputs
        keys = jnp.dot(frames, key_weight, preferred_element_type=jnp.float32).astype(jnp.bfloat16)
        values = jnp.dot(frames, value_weight, preferred_element_type=jnp.float32).astype(jnp.bfloat16)
        scores = jnp.dot(query_head, keys.T, preferred_element_type=jnp.float32) * HDIM ** (-0.5)
        peak = lax.optimization_barrier(jnp.max(scores, axis=1, keepdims=True))
        weights = jnp.exp(scores - peak)
        total = lax.optimization_barrier(jnp.sum(weights, axis=1, keepdims=True))
        mixed = jnp.dot(weights.astype(jnp.bfloat16), values, preferred_element_type=jnp.float32)
        return (mixed / total).astype(jnp.bfloat16)
    heads_out = lax.map(attend, (query_heads, key_weights, value_weights))
    attention = heads_out.transpose(1, 0, 2).reshape(LAT, INNER)
    latent_state = jnp.dot(attention, w_out, preferred_element_type=jnp.float32).astype(jnp.bfloat16)
    state_float = latent_state.astype(jnp.float32)
    scale_rows = lax.rsqrt(lax.optimization_barrier(jnp.mean(state_float * state_float, axis=1, keepdims=True)) + norm_eps)
    normed = (state_float * norm_gain[None, :]).astype(jnp.bfloat16)
    gate = jnp.dot(normed, w_gate, preferred_element_type=jnp.float32) * scale_rows
    up_part = jnp.dot(normed, w_up, preferred_element_type=jnp.float32) * scale_rows
    hidden = (jax.nn.silu(gate) * up_part).astype(jnp.bfloat16)
    down = jnp.dot(hidden, w_down, preferred_element_type=jnp.float32)
    return (state_float + down).astype(jnp.bfloat16)
```

```python
import jax
import jax.numpy as jnp
from jax import lax
from jax.sharding import Mesh
from jax.sharding import PartitionSpec as P

HDIM = 128
D = 8192
FRAMES = ("frames_0", "frames_1", "frames_2")
BF16 = jnp.bfloat16
F32 = jnp.float32


norm_eps = 1e-06


def exchange(blocks, axis):
    return lax.all_to_all(blocks, axis, split_axis=0, concat_axis=0, tiled=True)


def collect_rows(array, axis):
    peers = lax.axis_size(axis)
    blocks = exchange(jnp.broadcast_to(array[None], (peers, *array.shape)), axis)
    return blocks.reshape(peers * array.shape[0], *array.shape[1:])


def sum_rows_at_owner(array, axis):
    peers = lax.axis_size(axis)
    blocks = array.astype(BF16).reshape(peers, array.shape[0] // peers, *array.shape[1:])
    return jnp.sum(exchange(blocks, axis).astype(F32), axis=0)


def split_terms(array, count):
    terms = []
    for _ in range(count):
        term = lax.reduce_precision(array, 8, 7)
        terms.append(term.astype(BF16))
        array = array - term
    return terms


def joined_terms(terms):
    array = terms[-1].astype(F32)
    for term in terms[-2::-1]:
        array = array + term.astype(F32)
    return array


def merged_softmax(local_max, total, mixed):
    peers = lax.axis_size(FRAMES)
    rows, heads = local_max.shape
    share = rows // peers
    terms = jnp.stack(split_terms(local_max, 3) + split_terms(total, 3), axis=-1)
    stats = terms.reshape(peers, share * heads * 6)
    stats = jnp.pad(stats, ((0, 0), (0, -stats.shape[1] % HDIM))).reshape(peers, -1, HDIM)
    body = mixed.astype(BF16).reshape(peers, share * heads, HDIM)
    arrived = exchange(jnp.concatenate([body, stats], axis=1), FRAMES)
    body = arrived[:, : share * heads].reshape(peers, share, heads, HDIM).astype(F32)
    stats = arrived[:, share * heads :].reshape(peers, -1)[:, : share * heads * 6]
    stats = stats.reshape(peers, share, heads, 6)
    part_max = joined_terms([stats[..., k] for k in range(3)])
    part_total = joined_terms([stats[..., k] for k in range(3, 6)])
    scale = jnp.exp(part_max - jnp.max(part_max, axis=0))
    total = jnp.sum(part_total * scale, axis=0)
    mixed = jnp.sum(body * scale[..., None], axis=0)
    return (mixed / total[..., None]).reshape(share, heads * HDIM).astype(BF16)


def on_device(frames, latents, w_query, w_key, w_value, w_out, norm_gain, w_gate, w_up, w_down):
    local_query = jnp.dot(latents, w_query, preferred_element_type=F32).astype(BF16)
    queries = collect_rows(local_query, FRAMES)
    width = w_key.shape[1]
    piece = lax.all_gather(frames, "heads", axis=1, tiled=True)
    keys = jnp.dot(piece, w_key, preferred_element_type=F32)
    values = jnp.dot(piece, w_value, preferred_element_type=F32)
    heads_here = width // HDIM
    latent_count = queries.shape[0]
    query_heads = queries.reshape(latent_count, heads_here, HDIM)
    key_heads = keys.astype(BF16).reshape(-1, heads_here, HDIM)
    value_heads = values.astype(BF16).reshape(-1, heads_here, HDIM)
    scores = jnp.einsum(
        "qhd,khd->qhk", query_heads, key_heads, preferred_element_type=F32
    ) * HDIM ** (-0.5)
    local_max = jnp.max(scores, axis=2)
    weights = jnp.exp(scores - local_max[:, :, None])
    total = jnp.sum(weights, axis=2)
    mixed = jnp.einsum("qhk,khd->qhd", weights.astype(BF16), value_heads, preferred_element_type=F32)
    attention = collect_rows(merged_softmax(local_max, total, mixed), FRAMES)
    latent_state = sum_rows_at_owner(
        jnp.dot(attention, w_out, preferred_element_type=F32), "heads"
    ).astype(BF16)
    latent_full = collect_rows(latent_state, "heads")
    full_float = latent_full.astype(F32)
    square_part = jnp.sum(full_float * full_float, axis=1)
    normed = (full_float * norm_gain[None, :]).astype(BF16)
    gate_part = jnp.dot(normed, w_gate, preferred_element_type=F32).astype(BF16)
    up_part = jnp.dot(normed, w_up, preferred_element_type=F32).astype(BF16)
    square_terms = jnp.stack(split_terms(square_part, 2), axis=1)
    square_terms = jnp.pad(square_terms, ((0, 0), (0, 126)))
    peers = lax.axis_size(FRAMES)
    packed = jnp.concatenate([gate_part, up_part, square_terms], axis=1)
    sums = jnp.sum(exchange(packed.reshape(peers, -1, packed.shape[1]), FRAMES).astype(F32), axis=0)
    units = w_gate.shape[1]
    gate_sum, up_sum = sums[:, :units], sums[:, units : 2 * units]
    squares = sums[:, 2 * units : 2 * units + 1] + sums[:, 2 * units + 1 : 2 * units + 2]
    scale_rows = lax.rsqrt(squares / D + norm_eps)
    hidden = (jax.nn.silu(gate_sum * scale_rows) * (up_sum * scale_rows)).astype(BF16)
    hidden_full = collect_rows(hidden, FRAMES)
    down = sum_rows_at_owner(jnp.dot(hidden_full, w_down, preferred_element_type=F32), "heads")
    return (latent_state.astype(F32) + down).astype(BF16)


def solution(mesh):
    torus = Mesh(
        mesh.devices.reshape(4, 4, 2, mesh.shape["heads"]),
        ("frames_0", "frames_1", "frames_2", "heads"),
    )
    placed = (
        P(FRAMES, "heads"),
        P(FRAMES, None),
        P(None, "heads"),
        P(None, "heads"),
        P(None, "heads"),
        P("heads", FRAMES),
        P(FRAMES),
        P(FRAMES, "heads"),
        P(FRAMES, "heads"),
        P("heads", FRAMES),
    )
    return jax.shard_map(
        on_device, mesh=torus, in_specs=placed, out_specs=P("heads", FRAMES), check_vma=False
    )
```

```python
import jax
import jax.numpy as jnp
from jax import lax
from jax.sharding import Mesh
from jax.sharding import PartitionSpec as P

HDIM = 128
D = 8192
FRAMES = ("frames_0", "frames_1", "frames_2")
BF16 = jnp.bfloat16
F32 = jnp.float32


norm_eps = 1e-06
SCALE_STEPS = (64, 32, 16, 8, 4, 2)


def exchange(blocks, axis):
    return lax.all_to_all(blocks, axis, split_axis=0, concat_axis=0, tiled=True)


def collect_rows(array, axis):
    peers = lax.axis_size(axis)
    blocks = exchange(jnp.broadcast_to(array[None], (peers, *array.shape)), axis)
    return blocks.reshape(peers * array.shape[0], *array.shape[1:])


def sum_rows_at_owner(array, axis):
    peers = lax.axis_size(axis)
    blocks = array.astype(BF16).reshape(peers, array.shape[0] // peers, *array.shape[1:])
    return jnp.sum(exchange(blocks, axis).astype(F32), axis=0)


def split_terms(array, count):
    terms = []
    for _ in range(count):
        term = lax.reduce_precision(array, 8, 7)
        terms.append(term.astype(BF16))
        array = array - term
    return terms


def joined_terms(terms):
    array = terms[-1].astype(F32)
    for term in terms[-2::-1]:
        array = array + term.astype(F32)
    return array


def merged_softmax(local_max, total, mixed):
    peers = lax.axis_size(FRAMES)
    rows, heads = local_max.shape
    share = rows // peers
    terms = jnp.stack(split_terms(local_max, 3) + split_terms(total, 3), axis=-1)
    stats = terms.reshape(peers, share * heads * 6)
    stats = jnp.pad(stats, ((0, 0), (0, -stats.shape[1] % (2 * HDIM)))).reshape(peers, -1, HDIM)
    body = mixed.astype(BF16).reshape(peers, share * heads, HDIM)
    arrived = exchange(jnp.concatenate([body, stats], axis=1), FRAMES)
    body = arrived[:, : share * heads].reshape(peers, share, heads, HDIM).astype(F32)
    stats = arrived[:, share * heads :].reshape(peers, -1)[:, : share * heads * 6]
    stats = stats.reshape(peers, share, heads, 6)
    part_max = joined_terms([stats[..., k] for k in range(3)])
    part_total = joined_terms([stats[..., k] for k in range(3, 6)])
    scale = jnp.exp(part_max - jnp.max(part_max, axis=0))
    total = jnp.sum(part_total * scale, axis=0)
    mixed = jnp.sum(body * scale[..., None], axis=0)
    return (mixed / total[..., None]).reshape(share, heads * HDIM).astype(BF16)


def gathered_features(frames):
    block = frames.astype(F32)
    top = jnp.max(jnp.abs(block))
    scale = jnp.float32(1.0)
    taken = []
    for step in SCALE_STEPS:
        fits = top * 2.0**step <= 60000.0
        factor = jnp.where(fits, jnp.float32(2.0**step), jnp.float32(1.0))
        top = top * factor
        scale = scale * factor
        taken.append(jnp.where(fits, jnp.float32(1.0), jnp.float32(0.0)))
    taken += [jnp.float32(0.0)] * 2
    tokens, width = frames.shape
    flags = jnp.broadcast_to(jnp.stack(taken)[:, None], (len(taken), tokens))
    sent = jnp.concatenate([block.T * scale, flags], axis=0).astype(jnp.float16)
    arrived = lax.all_gather(sent, "heads", axis=0).astype(F32)
    inverse = jnp.ones((arrived.shape[0], 1, 1), F32)
    for k, step in enumerate(SCALE_STEPS):
        flag = arrived[:, width + k : width + k + 1, :1]
        inverse = inverse * jnp.where(flag > 0.5, jnp.float32(2.0**-step), jnp.float32(1.0))
    return (arrived[:, :width] * inverse).astype(BF16).reshape(-1, tokens)


def on_device(frames, latents, w_query, w_key, w_value, w_out, norm_gain, w_gate, w_up, w_down):
    local_query = jnp.dot(latents, w_query, preferred_element_type=F32).astype(BF16)
    queries = collect_rows(local_query, FRAMES)
    width = w_key.shape[1]
    piece = gathered_features(frames)
    keys = jnp.einsum("ft,fc->tc", piece, w_key, preferred_element_type=F32)
    values = jnp.einsum("ft,fc->tc", piece, w_value, preferred_element_type=F32)
    heads_here = width // HDIM
    latent_count = queries.shape[0]
    query_heads = queries.reshape(latent_count, heads_here, HDIM)
    key_heads = keys.astype(BF16).reshape(-1, heads_here, HDIM)
    value_heads = values.astype(BF16).reshape(-1, heads_here, HDIM)
    scores = jnp.einsum(
        "qhd,khd->qhk", query_heads, key_heads, preferred_element_type=F32
    ) * HDIM ** (-0.5)
    local_max = jnp.max(scores, axis=2)
    weights = jnp.exp(scores - local_max[:, :, None])
    total = jnp.sum(weights, axis=2)
    mixed = jnp.einsum("qhk,khd->qhd", weights.astype(BF16), value_heads, preferred_element_type=F32)
    attention = collect_rows(merged_softmax(local_max, total, mixed), FRAMES)
    latent_state = sum_rows_at_owner(
        jnp.dot(attention, w_out, preferred_element_type=F32), "heads"
    ).astype(BF16)
    latent_full = collect_rows(latent_state, "heads")
    full_float = latent_full.astype(F32)
    square_part = jnp.sum(full_float * full_float, axis=1)
    normed = (full_float * norm_gain[None, :]).astype(BF16)
    gate_part = jnp.dot(normed, w_gate, preferred_element_type=F32).astype(BF16)
    up_part = jnp.dot(normed, w_up, preferred_element_type=F32).astype(BF16)
    square_terms = jnp.stack(split_terms(square_part, 2), axis=1)
    square_terms = jnp.pad(square_terms, ((0, 0), (0, 126)))
    peers = lax.axis_size(FRAMES)
    packed = jnp.concatenate([gate_part, up_part, square_terms], axis=1)
    sums = jnp.sum(exchange(packed.reshape(peers, -1, packed.shape[1]), FRAMES).astype(F32), axis=0)
    units = w_gate.shape[1]
    gate_sum, up_sum = sums[:, :units], sums[:, units : 2 * units]
    squares = sums[:, 2 * units : 2 * units + 1] + sums[:, 2 * units + 1 : 2 * units + 2]
    scale_rows = lax.rsqrt(squares / D + norm_eps)
    hidden = (jax.nn.silu(gate_sum * scale_rows) * (up_sum * scale_rows)).astype(BF16)
    hidden_full = collect_rows(hidden, FRAMES)
    down = sum_rows_at_owner(jnp.dot(hidden_full, w_down, preferred_element_type=F32), "heads")
    return (latent_state.astype(F32) + down).astype(BF16)


def solution(mesh):
    torus = Mesh(
        mesh.devices.reshape(4, 4, 2, mesh.shape["heads"]),
        ("frames_0", "frames_1", "frames_2", "heads"),
    )
    placed = (
        P(FRAMES, "heads"),
        P(FRAMES, None),
        P(None, "heads"),
        P(None, "heads"),
        P(None, "heads"),
        P("heads", FRAMES),
        P(FRAMES),
        P(FRAMES, "heads"),
        P(FRAMES, "heads"),
        P("heads", FRAMES),
    )
    return jax.shard_map(
        on_device, mesh=torus, in_specs=placed, out_specs=P("heads", FRAMES), check_vma=False
    )
```

```python
import jax
import jax.numpy as jnp
from jax import lax
from jax.sharding import Mesh
from jax.sharding import PartitionSpec as P

HDIM = 128
D = 8192
FRAMES = ("frames_0", "frames_1", "frames_2")
CHIPS = ("frames_0", "frames_1")
CORE = "frames_2"
BF16 = jnp.bfloat16
F32 = jnp.float32


norm_eps = 1e-06
LANES = 128


def exchange(blocks, axis):
    return lax.all_to_all(blocks, axis, split_axis=0, concat_axis=0, tiled=True)


def collect_rows(array, axis):
    peers = lax.axis_size(axis)
    blocks = exchange(jnp.broadcast_to(array[None], (peers, *array.shape)), axis)
    return blocks.reshape(peers * array.shape[0], *array.shape[1:])


def sum_rows_at_owner(array, axis):
    peers = lax.axis_size(axis)
    blocks = array.astype(BF16).reshape(peers, array.shape[0] // peers, *array.shape[1:])
    return jnp.sum(exchange(blocks, axis).astype(F32), axis=0)


def split_terms(array, count):
    terms = []
    for _ in range(count):
        term = lax.reduce_precision(array, 8, 7)
        terms.append(term.astype(BF16))
        array = array - term
    return terms


def joined_terms(terms):
    array = terms[-1].astype(F32)
    for term in terms[-2::-1]:
        array = array + term.astype(F32)
    return array


def merged_softmax(local_max, total, mixed):
    peers = lax.axis_size(FRAMES)
    rows, heads = local_max.shape
    share = rows // peers
    terms = jnp.stack(split_terms(local_max, 3) + split_terms(total, 3), axis=-1)
    stats = terms.reshape(peers, share * heads * 6)
    stats = jnp.pad(stats, ((0, 0), (0, -stats.shape[1] % (2 * HDIM)))).reshape(peers, -1, HDIM)
    body = mixed.astype(BF16).reshape(peers, share * heads, HDIM)
    arrived = exchange(jnp.concatenate([body, stats], axis=1), FRAMES)
    body = arrived[:, : share * heads].reshape(peers, share, heads, HDIM).astype(F32)
    stats = arrived[:, share * heads :].reshape(peers, -1)[:, : share * heads * 6]
    stats = stats.reshape(peers, share, heads, 6)
    part_max = joined_terms([stats[..., k] for k in range(3)])
    part_total = joined_terms([stats[..., k] for k in range(3, 6)])
    scale = jnp.exp(part_max - jnp.max(part_max, axis=0))
    total = jnp.sum(part_total * scale, axis=0)
    mixed = jnp.sum(body * scale[..., None], axis=0)
    return (mixed / total[..., None]).reshape(share, heads * HDIM).astype(BF16)


def power_near(value):
    return lax.reduce_precision(value, 8, 0)


def gathered_features(frames):
    tokens, width = frames.shape
    top = jnp.maximum(jnp.max(jnp.abs(frames)).astype(F32), 2.0**-108)
    exponent = jnp.round(jnp.log2(top))
    scale = power_near(jnp.exp2(14.0 - exponent))
    groups = tokens // LANES
    block = frames.astype(F32).T.reshape(width, groups, LANES).transpose(1, 0, 2) * scale
    tail = jnp.broadcast_to(exponent, (8, LANES))
    sent = jnp.concatenate([block.reshape(-1, LANES), tail], axis=0).astype(jnp.float16)
    arrived = lax.all_gather(sent.reshape(-1, 8, LANES), "heads", axis=0)
    peers = arrived.shape[0]
    inverse = power_near(jnp.exp2(arrived[:, width, :1, :1].astype(F32) - 14.0))
    features = arrived[:, :width].reshape(peers, groups, width, LANES).astype(F32)
    features = (features * inverse[:, None]).astype(BF16)
    return features.transpose(0, 2, 1, 3).reshape(peers * width, tokens)


def on_device(frames, latents, w_query, w_key, w_value, w_out, norm_gain, w_gate, w_up, w_down):
    local_query = jnp.dot(latents, w_query, preferred_element_type=F32).astype(BF16)
    queries = collect_rows(local_query, FRAMES)
    width = w_key.shape[1]
    piece = gathered_features(frames)
    keys = jnp.einsum("ft,fc->tc", piece, w_key, preferred_element_type=F32)
    values = jnp.einsum("ft,fc->tc", piece, w_value, preferred_element_type=F32)
    heads_here = width // HDIM
    latent_count = queries.shape[0]
    query_heads = queries.reshape(latent_count, heads_here, HDIM)
    key_heads = keys.astype(BF16).reshape(-1, heads_here, HDIM)
    value_heads = values.astype(BF16).reshape(-1, heads_here, HDIM)
    scores = jnp.einsum(
        "qhd,khd->qhk", query_heads, key_heads, preferred_element_type=F32
    ) * HDIM ** (-0.5)
    local_max = jnp.max(scores, axis=2)
    weights = jnp.exp(scores - local_max[:, :, None])
    total = jnp.sum(weights, axis=2)
    mixed = jnp.einsum("qhk,khd->qhd", weights.astype(BF16), value_heads, preferred_element_type=F32)
    attention = collect_rows(merged_softmax(local_max, total, mixed), FRAMES)
    latent_state = sum_rows_at_owner(
        jnp.dot(attention, w_out, preferred_element_type=F32), "heads"
    ).astype(BF16)
    latent_full = collect_rows(latent_state, "heads")
    full_float = latent_full.astype(F32)
    normed = (full_float * norm_gain[None, :]).astype(BF16)
    square_part = jnp.sum(full_float * full_float, axis=1, keepdims=True)
    units = w_gate.shape[1]
    core = lax.axis_index(CORE)
    share = latent_count // lax.axis_size(FRAMES)

    def rows_of(array, owner):
        blocks = array.reshape(lax.axis_size(CHIPS), 2, share, array.shape[1])
        return lax.dynamic_index_in_dim(blocks, owner, 1, keepdims=False).reshape(-1, array.shape[1])

    def partial_sums(owner):
        rows = rows_of(normed, owner)
        gate = jnp.dot(rows, w_gate, preferred_element_type=F32)
        up = jnp.dot(rows, w_up, preferred_element_type=F32)
        return gate, up, rows_of(square_part, owner)

    def packed(gate, up, squares):
        terms = jnp.pad(jnp.concatenate(split_terms(squares, 2), axis=1), ((0, 0), (0, 126)))
        return jnp.concatenate([gate.astype(BF16), up.astype(BF16), terms], axis=1)

    def unpacked(sums):
        squares = sums[:, 2 * units : 2 * units + 1] + sums[:, 2 * units + 1 : 2 * units + 2]
        return sums[:, :units], sums[:, units : 2 * units], squares

    handed = lax.ppermute(packed(*partial_sums(1 - core)), CORE, [(0, 1), (1, 0)])
    theirs = unpacked(handed.astype(F32))
    blocks = packed(*[a + b for a, b in zip(partial_sums(core), theirs)])
    blocks = exchange(blocks.reshape(-1, share, blocks.shape[1]), CHIPS)
    gate_sum, up_sum, squares = unpacked(jnp.sum(blocks.astype(F32), axis=0))
    scale_rows = lax.rsqrt(squares / D + norm_eps)
    hidden = (jax.nn.silu(gate_sum * scale_rows) * (up_sum * scale_rows)).astype(BF16)
    hidden_full = collect_rows(hidden, FRAMES)
    down = sum_rows_at_owner(jnp.dot(hidden_full, w_down, preferred_element_type=F32), "heads")
    return (latent_state.astype(F32) + down).astype(BF16)


def solution(mesh):
    torus = Mesh(
        mesh.devices.reshape(4, 4, 2, mesh.shape["heads"]),
        ("frames_0", "frames_1", "frames_2", "heads"),
    )
    placed = (
        P(FRAMES, "heads"),
        P(FRAMES, None),
        P(None, "heads"),
        P(None, "heads"),
        P(None, "heads"),
        P("heads", FRAMES),
        P(FRAMES),
        P(FRAMES, "heads"),
        P(FRAMES, "heads"),
        P("heads", FRAMES),
    )
    return jax.shard_map(
        on_device, mesh=torus, in_specs=placed, out_specs=P("heads", FRAMES), check_vma=False
    )
```

```python
import jax
import jax.numpy as jnp
from jax import lax
from jax.sharding import Mesh
from jax.sharding import PartitionSpec as P

HDIM = 128
D = 8192
FRAMES = ("frames_0", "frames_1", "frames_2")
CHIPS = ("frames_0", "frames_1")
CORE = "frames_2"
BF16 = jnp.bfloat16
F32 = jnp.float32


norm_eps = 1e-06
LANES = 128


def exchange(blocks, axis):
    return lax.all_to_all(blocks, axis, split_axis=0, concat_axis=0, tiled=True)


def collect_rows(array, axis):
    peers = lax.axis_size(axis)
    blocks = exchange(jnp.broadcast_to(array[None], (peers, *array.shape)), axis)
    return blocks.reshape(peers * array.shape[0], *array.shape[1:])


def sum_rows_at_owner(array, axis):
    peers = lax.axis_size(axis)
    blocks = array.astype(BF16).reshape(peers, array.shape[0] // peers, *array.shape[1:])
    return jnp.sum(exchange(blocks, axis).astype(F32), axis=0)


def split_terms(array, count):
    terms = []
    for _ in range(count):
        term = lax.reduce_precision(array, 8, 7)
        terms.append(term.astype(BF16))
        array = array - term
    return terms


def joined_terms(terms):
    array = terms[-1].astype(F32)
    for term in terms[-2::-1]:
        array = array + term.astype(F32)
    return array


def merged_softmax(local_max, total, mixed):
    peers = lax.axis_size(FRAMES)
    rows, heads = local_max.shape
    share = rows // peers
    terms = jnp.stack(split_terms(local_max, 3) + split_terms(total, 3), axis=-1)
    stats = terms.reshape(peers, share * heads * 6)
    stats = jnp.pad(stats, ((0, 0), (0, -stats.shape[1] % (2 * HDIM)))).reshape(peers, -1, HDIM)
    body = mixed.astype(BF16).reshape(peers, share * heads, HDIM)
    arrived = exchange(jnp.concatenate([body, stats], axis=1), FRAMES)
    body = arrived[:, : share * heads].reshape(peers, share, heads, HDIM).astype(F32)
    stats = arrived[:, share * heads :].reshape(peers, -1)[:, : share * heads * 6]
    stats = stats.reshape(peers, share, heads, 6)
    part_max = joined_terms([stats[..., k] for k in range(3)])
    part_total = joined_terms([stats[..., k] for k in range(3, 6)])
    scale = jnp.exp(part_max - jnp.max(part_max, axis=0))
    total = jnp.sum(part_total * scale, axis=0)
    mixed = jnp.sum(body * scale[..., None], axis=0)
    return (mixed / total[..., None]).reshape(share, heads * HDIM).astype(BF16)


def power_near(value):
    return lax.reduce_precision(value, 8, 0)


def gathered_features(frames):
    tokens, width = frames.shape
    groups = tokens // LANES
    block = lax.optimization_barrier(frames.astype(F32).T)
    top = jnp.max(jnp.max(jnp.abs(block).reshape(-1, 8, tokens), axis=0).reshape(8, groups, LANES), axis=1)
    top = lax.optimization_barrier(jnp.max(top, keepdims=True))
    top = jnp.maximum(jnp.broadcast_to(top, (8, LANES)), 2.0**-108)
    exponent = lax.optimization_barrier(jnp.round(jnp.log2(top)))
    scale = power_near(jnp.exp2(14.0 - exponent))
    block = (block.reshape(-1, 8, groups, LANES) * scale[:, None]).astype(jnp.float16)
    block = block.transpose(2, 0, 1, 3).reshape(-1, LANES)
    sent = jnp.concatenate([block, exponent.astype(jnp.float16)], axis=0)
    arrived = lax.all_gather(sent.reshape(-1, 8, LANES), "heads", axis=0)
    peers = arrived.shape[0]
    inverse = power_near(jnp.exp2(arrived[:, width, :1, :1].astype(F32) - 14.0))
    features = arrived[:, :width].reshape(peers, groups, width, LANES).astype(F32)
    features = (features * inverse[:, None]).astype(BF16)
    return features.transpose(0, 2, 1, 3).reshape(peers * width, tokens)


def on_device(frames, latents, w_query, w_key, w_value, w_out, norm_gain, w_gate, w_up, w_down):
    core = lax.convert_element_type(lax.axis_index(CORE), jnp.uint32)
    core, other, latents = lax.optimization_barrier((core, jnp.uint32(1) - core, latents))
    local_query = jnp.dot(latents, w_query, preferred_element_type=F32).astype(BF16)
    queries = collect_rows(local_query, FRAMES)
    width = w_key.shape[1]
    piece = gathered_features(frames)
    keys = jnp.einsum("ft,fc->tc", piece, w_key, preferred_element_type=F32)
    values = jnp.einsum("ft,fc->tc", piece, w_value, preferred_element_type=F32)
    heads_here = width // HDIM
    latent_count = queries.shape[0]
    query_heads = queries.reshape(latent_count, heads_here, HDIM)
    key_heads = keys.astype(BF16).reshape(-1, heads_here, HDIM)
    value_heads = values.astype(BF16).reshape(-1, heads_here, HDIM)
    scores = jnp.einsum(
        "qhd,khd->qhk", query_heads, key_heads, preferred_element_type=F32
    ) * HDIM ** (-0.5)
    local_max = jnp.max(scores, axis=2)
    weights = jnp.exp(scores - local_max[:, :, None])
    total = jnp.sum(weights, axis=2)
    mixed = jnp.einsum("qhk,khd->qhd", weights.astype(BF16), value_heads, preferred_element_type=F32)
    attention = collect_rows(merged_softmax(local_max, total, mixed), FRAMES)
    latent_state = sum_rows_at_owner(
        jnp.dot(attention, w_out, preferred_element_type=F32), "heads"
    ).astype(BF16)
    latent_full = collect_rows(latent_state, "heads")
    full_float = latent_full.astype(F32)
    normed = (full_float * norm_gain[None, :]).astype(BF16)
    square_part = jnp.sum(full_float * full_float, axis=1, keepdims=True)
    units = w_gate.shape[1]
    share = latent_count // lax.axis_size(FRAMES)

    def rows_of(array, owner):
        blocks = array.reshape(lax.axis_size(CHIPS), 2, share, array.shape[1])
        return lax.dynamic_index_in_dim(blocks, owner, 1, keepdims=False).reshape(-1, array.shape[1])

    def partial_sums(owner):
        rows = rows_of(normed, owner)
        gate = jnp.dot(rows, w_gate, preferred_element_type=F32)
        up = jnp.dot(rows, w_up, preferred_element_type=F32)
        return gate, up, rows_of(square_part, owner)

    def packed(gate, up, squares):
        terms = jnp.pad(jnp.concatenate(split_terms(squares, 2), axis=1), ((0, 0), (0, 126)))
        return jnp.concatenate([gate.astype(BF16), up.astype(BF16), terms], axis=1)

    def unpacked(sums):
        squares = sums[:, 2 * units : 2 * units + 1] + sums[:, 2 * units + 1 : 2 * units + 2]
        return sums[:, :units], sums[:, units : 2 * units], squares

    handed = lax.ppermute(packed(*partial_sums(other)), CORE, [(0, 1), (1, 0)])
    theirs = unpacked(handed.astype(F32))
    blocks = packed(*[a + b for a, b in zip(partial_sums(core), theirs)])
    blocks = exchange(blocks.reshape(-1, share, blocks.shape[1]), CHIPS)
    gate_sum, up_sum, squares = unpacked(jnp.sum(blocks.astype(F32), axis=0))
    scale_rows = lax.rsqrt(squares / D + norm_eps)
    hidden = (jax.nn.silu(gate_sum * scale_rows) * (up_sum * scale_rows)).astype(BF16)
    hidden_full = collect_rows(hidden, FRAMES)
    down = sum_rows_at_owner(jnp.dot(hidden_full, w_down, preferred_element_type=F32), "heads")
    return (latent_state.astype(F32) + down).astype(BF16)


def solution(mesh):
    torus = Mesh(
        mesh.devices.reshape(4, 4, 2, mesh.shape["heads"]),
        ("frames_0", "frames_1", "frames_2", "heads"),
    )
    placed = (
        P(FRAMES, "heads"),
        P(FRAMES, None),
        P(None, "heads"),
        P(None, "heads"),
        P(None, "heads"),
        P("heads", FRAMES),
        P(FRAMES),
        P(FRAMES, "heads"),
        P(FRAMES, "heads"),
        P("heads", FRAMES),
    )
    return jax.shard_map(
        on_device, mesh=torus, in_specs=placed, out_specs=P("heads", FRAMES), check_vma=False
    )
```

```python
import jax
import jax.numpy as jnp
from jax import lax
from jax.sharding import Mesh
from jax.sharding import PartitionSpec as P

HDIM = 128
D = 8192
FRAMES = ("frames_0", "frames_1", "frames_2")
CHIPS = ("frames_0", "frames_1")
CORE = "frames_2"
BF16 = jnp.bfloat16
F32 = jnp.float32


norm_eps = 1e-06
LANES = 128


def exchange(blocks, axis):
    return lax.all_to_all(blocks, axis, split_axis=0, concat_axis=0, tiled=True)


def collect_rows(array, axis):
    peers = lax.axis_size(axis)
    blocks = exchange(jnp.broadcast_to(array[None], (peers, *array.shape)), axis)
    return blocks.reshape(peers * array.shape[0], *array.shape[1:])


def sum_rows_at_owner(array, axis):
    peers = lax.axis_size(axis)
    blocks = array.astype(BF16).reshape(peers, array.shape[0] // peers, *array.shape[1:])
    return jnp.sum(exchange(blocks, axis).astype(F32), axis=0)


def split_terms(array, count):
    terms = []
    for _ in range(count):
        term = lax.reduce_precision(array, 8, 7)
        terms.append(term.astype(BF16))
        array = array - term
    return terms


def joined_terms(terms):
    array = terms[-1].astype(F32)
    for term in terms[-2::-1]:
        array = array + term.astype(F32)
    return array


def merged_softmax(local_max, total, mixed):
    peers = lax.axis_size(FRAMES)
    rows, heads = local_max.shape
    share = rows // peers
    terms = jnp.stack(split_terms(local_max, 3) + split_terms(total, 3), axis=-1)
    stats = terms.reshape(peers, share * heads * 6)
    stats = jnp.pad(stats, ((0, 0), (0, -stats.shape[1] % (2 * HDIM)))).reshape(peers, -1, HDIM)
    body = mixed.astype(BF16).reshape(peers, share * heads, HDIM)
    arrived = exchange(jnp.concatenate([body, stats], axis=1), FRAMES)
    body = arrived[:, : share * heads].reshape(peers, share, heads, HDIM).astype(F32)
    stats = arrived[:, share * heads :].reshape(peers, -1)[:, : share * heads * 6]
    stats = stats.reshape(peers, share, heads, 6)
    part_max = joined_terms([stats[..., k] for k in range(3)])
    part_total = joined_terms([stats[..., k] for k in range(3, 6)])
    scale = jnp.exp(part_max - jnp.max(part_max, axis=0))
    total = jnp.sum(part_total * scale, axis=0)
    mixed = jnp.sum(body * scale[..., None], axis=0)
    return (mixed / total[..., None]).reshape(share, heads * HDIM).astype(BF16)


def power_near(value):
    return lax.reduce_precision(value, 8, 0)


def gathered_features(frames):
    tokens, width = frames.shape
    groups = tokens // LANES
    block = lax.optimization_barrier(frames.astype(F32).T)
    top = jnp.max(jnp.max(jnp.abs(block).reshape(-1, 8, tokens), axis=0).reshape(8, groups, LANES), axis=1)
    top = lax.optimization_barrier(jnp.max(top, keepdims=True))
    top = jnp.maximum(jnp.broadcast_to(top, (8, LANES)), 2.0**-108)
    exponent = lax.optimization_barrier(jnp.round(jnp.log2(top)))
    scale = power_near(jnp.exp2(14.0 - exponent))
    block = (block.reshape(-1, 8, groups, LANES) * scale[:, None]).astype(jnp.float16)
    block = block.transpose(2, 0, 1, 3).reshape(-1, LANES)
    sent = jnp.concatenate([block, exponent.astype(jnp.float16)], axis=0)
    arrived = lax.all_gather(sent.reshape(-1, 8, LANES), "heads", axis=0)
    peers = arrived.shape[0]
    inverse = power_near(jnp.exp2(arrived[:, width, :1, :1].astype(F32) - 14.0))
    features = arrived[:, :width].reshape(peers, groups, width, LANES).astype(F32)
    features = (features * inverse[:, None]).astype(BF16)
    return features.transpose(0, 2, 1, 3).reshape(peers * width, tokens)


def on_device(frames, latents, w_query, w_key, w_value, w_out, norm_gain, w_gate, w_up, w_down):
    core = lax.convert_element_type(lax.axis_index(CORE), jnp.uint32)
    core, other, latents = lax.optimization_barrier((core, jnp.uint32(1) - core, latents))
    local_query = jnp.dot(latents, w_query, preferred_element_type=F32).astype(BF16)
    queries = collect_rows(local_query, FRAMES)
    width = w_key.shape[1]
    piece = gathered_features(frames)
    keys = jnp.einsum("ft,fc->tc", piece, w_key, preferred_element_type=F32)
    values = jnp.einsum("ft,fc->tc", piece, w_value, preferred_element_type=F32)
    heads_here = width // HDIM
    latent_count = queries.shape[0]
    query_heads = queries.reshape(latent_count, heads_here, HDIM)
    key_heads = keys.astype(BF16).reshape(-1, heads_here, HDIM)
    value_heads = values.astype(BF16).reshape(-1, heads_here, HDIM)
    scores = jnp.einsum(
        "qhd,khd->qhk", query_heads, key_heads, preferred_element_type=F32
    ) * HDIM ** (-0.5)
    local_max = jnp.max(scores, axis=2)
    weights = jnp.exp(scores - local_max[:, :, None])
    total = jnp.sum(weights, axis=2)
    mixed = jnp.einsum("qhk,khd->qhd", weights.astype(BF16), value_heads, preferred_element_type=F32)
    attention = collect_rows(merged_softmax(local_max, total, mixed), FRAMES)
    latent_state = sum_rows_at_owner(
        jnp.dot(attention, w_out, preferred_element_type=F32), "heads"
    ).astype(BF16)
    latent_full = collect_rows(latent_state, "heads")
    full_float = latent_full.astype(F32)
    normed = (full_float * norm_gain[None, :]).astype(BF16)
    square_part = jnp.sum(full_float * full_float, axis=1, keepdims=True)
    units = w_gate.shape[1]
    share = latent_count // lax.axis_size(FRAMES)

    def rows_of(array, owner):
        blocks = array.reshape(lax.axis_size(CHIPS), 2, share, array.shape[1])
        return lax.dynamic_index_in_dim(blocks, owner, 1, keepdims=False).reshape(-1, array.shape[1])

    def partial_sums(owner):
        rows = rows_of(normed, owner)
        gate = jnp.dot(rows, w_gate, preferred_element_type=F32)
        up = jnp.dot(rows, w_up, preferred_element_type=F32)
        return gate, up, rows_of(square_part, owner)

    def packed(gate, up, squares):
        terms = jnp.pad(jnp.concatenate(split_terms(squares, 2), axis=1), ((0, 0), (0, 126)))
        return jnp.concatenate([gate.astype(BF16), up.astype(BF16), terms], axis=1)

    def squares_in(array):
        terms = array[:, 2 * units : 2 * units + 2].astype(F32)
        return terms[:, :1] + terms[:, 1:]

    handed = lax.ppermute(packed(*partial_sums(other)), CORE, [(0, 1), (1, 0)])
    gate, up, squares = lax.optimization_barrier(partial_sums(core))
    gate = gate + handed[:, :units].astype(F32)
    up = up + handed[:, units : 2 * units].astype(F32)
    blocks = packed(gate, up, squares + squares_in(handed))
    blocks = exchange(blocks.reshape(-1, share, blocks.shape[1]), CHIPS)
    sums = jnp.sum(blocks.astype(F32), axis=0)
    gate_sum, up_sum, squares = sums[:, :units], sums[:, units : 2 * units], squares_in(sums)
    scale_rows = lax.rsqrt(squares / D + norm_eps)
    hidden = (jax.nn.silu(gate_sum * scale_rows) * (up_sum * scale_rows)).astype(BF16)
    hidden_full = collect_rows(hidden, FRAMES)
    down = sum_rows_at_owner(jnp.dot(hidden_full, w_down, preferred_element_type=F32), "heads")
    return (latent_state.astype(F32) + down).astype(BF16)


def solution(mesh):
    torus = Mesh(
        mesh.devices.reshape(4, 4, 2, mesh.shape["heads"]),
        ("frames_0", "frames_1", "frames_2", "heads"),
    )
    placed = (
        P(FRAMES, "heads"),
        P(FRAMES, None),
        P(None, "heads"),
        P(None, "heads"),
        P(None, "heads"),
        P("heads", FRAMES),
        P(FRAMES),
        P(FRAMES, "heads"),
        P(FRAMES, "heads"),
        P("heads", FRAMES),
    )
    return jax.shard_map(
        on_device, mesh=torus, in_specs=placed, out_specs=P("heads", FRAMES), check_vma=False
    )
```
